32 devices in a mesh: batch: 1 (over z), stage: 4 (over y), seq: 8 (over x, core).
Axes of the slice: x: 4, y: 4, z: 1, core: 2. Of those that a mesh axis runs over, the one named last changes fastest.
The devices are a block of a 4x4x8 slice.
Arguments:
- x_tokens: bfloat16 [2, 8192, 1024], P('batch', 'seq')
- norm_attn: bfloat16 [4, 1024], P('stage')
- w_query: bfloat16 [4, 1024, 4096], P('stage')
- w_key: bfloat16 [4, 1024, 4096], P('stage')
- w_value: bfloat16 [4, 1024, 2048], P('stage')
- w_gate: bfloat16 [4, 1024, 32], P('stage')
- gate_bias: float32 [4, 32], P('stage')
- norm_out: bfloat16 [4, 64], P('stage')
- w_out: bfloat16 [4, 2048, 1024], P('stage')
- norm_mlp: bfloat16 [4, 1024], P('stage')
- w_up: bfloat16 [4, 1024, 4096], P('stage')
- w_down: bfloat16 [4, 4096, 1024], P('stage')
Outputs:
- output 1: bfloat16 [4, 2, 8192, 1024], P('stage', 'batch', 'seq')
- output 2: float32 [4, 2, 32, 128, 64], P('stage', 'batch')
All inputs are finite; a program needn't handle non-finite values.
Results may differ from the reference program's by a relative error of at most 0.02.
Values are sent between devices in bfloat16 or wider.
A program may use at most 768 MiB of HBM per device.

```python
import math
import jax
import jax.numpy as jnp
from jax import lax

NUM_SEQS = 2
CHUNK_LEN = 1024
TOKENS = 8192
MODEL_DIM = 1024
NUM_HEADS = 32
KEY_DIM = 128
VAL_DIM = 64
FFN_DIM = 4096
LAYERS = 4
NORM_EPS = 1e-6
NUM_CHUNKS = TOKENS // CHUNK_LEN
TOTAL_ROWS = NUM_SEQS * TOKENS


def dense_weight(rng_key, fan_in, fan_out):
    raw_draw = jax.random.normal(rng_key, (LAYERS, fan_in, fan_out), jnp.float32)
    return (raw_draw * fan_in ** -0.5).astype(jnp.bfloat16)


def gain_vector(rng_key, vec_width):
    raw_draw = jax.random.normal(rng_key, (LAYERS, vec_width), jnp.float32)
    return (1.0 + 0.3 * raw_draw).astype(jnp.bfloat16)


def setup_inputs(seed: int = 0, part: int = 0) -> dict:
    base_key = jax.random.key(seed)
    token_keys = jax.random.split(jax.random.fold_in(base_key, part), 2)
    weight_keys = jax.random.split(base_key, 11)
    token_noise = jax.random.normal(token_keys[0], (NUM_SEQS, TOKENS, MODEL_DIM), jnp.float32)
    walk_steps = jax.random.normal(token_keys[1], (NUM_SEQS, TOKENS, MODEL_DIM), jnp.float32)
    token_drift = jnp.cumsum(walk_steps, axis=1) * TOKENS ** -0.5
    gate_bias = math.log(CHUNK_LEN) + jax.random.uniform(weight_keys[5], (LAYERS, NUM_HEADS), jnp.float32, 0.0, 1.5)
    return {
        'x_tokens': (token_noise + 0.7 * token_drift).astype(jnp.bfloat16),
        'norm_attn': gain_vector(weight_keys[0], MODEL_DIM),
        'w_query': dense_weight(weight_keys[1], MODEL_DIM, NUM_HEADS * KEY_DIM),
        'w_key': dense_weight(weight_keys[2], MODEL_DIM, NUM_HEADS * KEY_DIM),
        'w_value': dense_weight(weight_keys[3], MODEL_DIM, NUM_HEADS * VAL_DIM),
        'w_gate': dense_weight(weight_keys[4], MODEL_DIM, NUM_HEADS),
        'gate_bias': gate_bias,
        'norm_out': gain_vector(weight_keys[6], VAL_DIM),
        'w_out': dense_weight(weight_keys[7], NUM_HEADS * VAL_DIM, MODEL_DIM),
        'norm_mlp': gain_vector(weight_keys[8], MODEL_DIM),
        'w_up': dense_weight(weight_keys[9], MODEL_DIM, FFN_DIM),
        'w_down': dense_weight(weight_keys[10], FFN_DIM, MODEL_DIM),
    }


def rms_norm(values, gain_vec):
    mean_sq = jnp.mean(values * values, axis=-1, keepdims=True)
    return values * lax.rsqrt(mean_sq + NORM_EPS) * gain_vec.astype(jnp.float32)


def chunk_step(carry_state, chunk_in):
    q_blk, k_blk, v_blk, decay_blk = chunk_in
    cum_decay = jnp.cumsum(decay_blk, axis=1)
    total_decay = cum_decay[:, -1, :]
    q_f32 = q_blk.astype(jnp.float32)
    k_f32 = k_blk.astype(jnp.float32)
    v_f32 = v_blk.astype(jnp.float32)
    inter_out = jnp.einsum('schk,shkv->schv', q_f32, carry_state) * jnp.exp(cum_decay)[..., None]
    scores = jnp.einsum('schk,sjhk->shcj', q_f32, k_f32)
    cum_heads = jnp.swapaxes(cum_decay, 1, 2)
    causal = jnp.arange(CHUNK_LEN)[:, None] >= jnp.arange(CHUNK_LEN)[None, :]
    decay_mat = jnp.exp(jnp.where(causal, cum_heads[:, :, :, None] - cum_heads[:, :, None, :], -jnp.inf))
    intra_out = jnp.einsum('shcj,sjhv->schv', scores * decay_mat, v_f32)
    k_decayed = k_f32 * jnp.exp(total_decay[:, None, :] - cum_decay)[..., None]
    new_state = jnp.exp(total_decay)[:, :, None, None] * carry_state + jnp.einsum('sjhk,sjhv->shkv', k_decayed, v_f32)
    return new_state, inter_out + intra_out


def to_chunks(values):
    shaped = values.reshape((NUM_SEQS, NUM_CHUNKS, CHUNK_LEN) + values.shape[1:])
    return jnp.moveaxis(shaped, 1, 0)


def layer_step(h_in, params):
    norm_attn, w_query, w_key, w_value, w_gate, gate_bias, norm_out, w_out, norm_mlp, w_up, w_down = params
    h_f32 = h_in.astype(jnp.float32).reshape(TOTAL_ROWS, MODEL_DIM)
    u_norm = rms_norm(h_f32, norm_attn).astype(jnp.bfloat16)
    q_all = jnp.dot(u_norm, w_query, preferred_element_type=jnp.float32).astype(jnp.bfloat16)
    k_all = (jnp.dot(u_norm, w_key, preferred_element_type=jnp.float32) * KEY_DIM ** -0.5).astype(jnp.bfloat16)
    v_all = jnp.dot(u_norm, w_value, preferred_element_type=jnp.float32).astype(jnp.bfloat16)
    log_decay = jax.nn.log_sigmoid(jnp.dot(u_norm, w_gate, preferred_element_type=jnp.float32) + gate_bias)
    chunks_in = (
        to_chunks(q_all.reshape(TOTAL_ROWS, NUM_HEADS, KEY_DIM)),
        to_chunks(k_all.reshape(TOTAL_ROWS, NUM_HEADS, KEY_DIM)),
        to_chunks(v_all.reshape(TOTAL_ROWS, NUM_HEADS, VAL_DIM)),
        to_chunks(log_decay),
    )
    zero_state = jnp.zeros((NUM_SEQS, NUM_HEADS, KEY_DIM, VAL_DIM), jnp.float32)
    final_state, chunk_outs = lax.scan(chunk_step, zero_state, chunks_in)
    attn_out = jnp.moveaxis(chunk_outs, 0, 1).reshape(TOTAL_ROWS, NUM_HEADS, VAL_DIM)
    head_norm = rms_norm(attn_out, norm_out).astype(jnp.bfloat16).reshape(TOTAL_ROWS, NUM_HEADS * VAL_DIM)
    h_mid = h_f32 + jnp.dot(head_norm, w_out, preferred_element_type=jnp.float32)
    mlp_in = rms_norm(h_mid, norm_mlp).astype(jnp.bfloat16)
    hidden = jax.nn.gelu(jnp.dot(mlp_in, w_up, preferred_element_type=jnp.float32), approximate=True).astype(jnp.bfloat16)
    h_out = (h_mid + jnp.dot(hidden, w_down, preferred_element_type=jnp.float32)).astype(jnp.bfloat16)
    h_out = h_out.reshape(NUM_SEQS, TOKENS, MODEL_DIM)
    return h_out, (h_out, final_state)


def reference(x_tokens, norm_attn, w_query, w_key, w_value, w_gate, gate_bias, norm_out, w_out, norm_mlp, w_up, w_down):
    params = (norm_attn, w_query, w_key, w_value, w_gate, gate_bias, norm_out, w_out, norm_mlp, w_up, w_down)
    last_h, (y_layers, s_final) = lax.scan(layer_step, x_tokens, params)
    return y_layers, s_final
```

```python
import functools

import jax
import jax.numpy as jnp
from jax import lax
from jax.experimental import pallas as pl
from jax.experimental.pallas import tpu as pltpu
from jax.sharding import PartitionSpec as P

NORM_EPS = 1e-6
CHUNK = 256
PAIRS = 4
PIECES = 2
COLS = 256
ROWS = 256
HIDDEN = 512
LINKS = 8


def rms_norm(values, gain_vec):
    mean_sq = jnp.mean(values * values, axis=-1, keepdims=True)
    return values * lax.rsqrt(mean_sq + NORM_EPS) * gain_vec.astype(jnp.float32)


def dot_f32(lhs, rhs):
    return jnp.dot(lhs, rhs, preferred_element_type=jnp.float32)


def project_kernel(key_dim, chunk, h_ref, norm_ref, wg_ref, bias_ref, tri_ref, wq_ref, wk_ref, wv_ref, sin_ref,
                   q_ref, kt_ref, v_ref, cum_ref, sout_ref, u_scr, cum_scr):
    rows = h_ref.shape[0]
    heads = cum_ref.shape[0]
    group = pl.program_id(0)

    @pl.when(group == 0)
    def _():
        u_scr[...] = rms_norm(h_ref[...].astype(jnp.float32), norm_ref[...]).astype(jnp.bfloat16)
        gate = lax.dot_general(wg_ref[...], u_scr[...], (((1,), (1,)), ((), ())), preferred_element_type=jnp.float32)
        log_decay = jax.nn.log_sigmoid(gate + bias_ref[...])
        for start in range(0, rows, chunk):
            cum_scr[:, start:start + chunk] = jnp.dot(
                log_decay[:, start:start + chunk], tri_ref[...], precision=lax.Precision.HIGHEST,
                preferred_element_type=jnp.float32)

    u_norm = u_scr[...]
    for start in range(0, wv_ref.shape[1], COLS):
        v_ref[:, start:start + COLS] = dot_f32(u_norm, wv_ref[:, start:start + COLS]).astype(jnp.bfloat16)
    for start in range(0, wk_ref.shape[1], COLS):
        k_part = dot_f32(u_norm, wk_ref[:, start:start + COLS]) * key_dim ** -0.5
        kt_ref[start:start + COLS, :] = k_part.T.astype(jnp.bfloat16)
    for start in range(0, wq_ref.shape[1], COLS):
        q_ref[:, start:start + COLS] = dot_f32(u_norm, wq_ref[:, start:start + COLS]).astype(jnp.bfloat16)

    cum = cum_scr[pl.ds(pl.multiple_of(group * heads, heads), heads), :]
    cum_ref[...] = cum
    total = jnp.zeros((heads, 1), jnp.float32)
    rest = []
    for start in range(rows - chunk, -1, -chunk):
        last = cum[:, start + chunk - 1:start + chunk]
        rest.insert(0, total + (last - cum[:, start:start + chunk]))
        total = total + last
    weight = jnp.exp(jnp.concatenate(rest, axis=1))
    total = jnp.exp(total)
    wide = sout_ref.shape[2]
    low = lax.broadcasted_iota(jnp.int32, (key_dim, wide), 1) < wide // 2
    for pair in range(sout_ref.shape[0]):
        v_pair = v_ref[:, pair * wide:(pair + 1) * wide]
        state = sin_ref[pair]
        parts = []
        for head in (2 * pair, 2 * pair + 1):
            k_t = kt_ref[head * key_dim:(head + 1) * key_dim, :].astype(jnp.float32)
            parts.append(total[head:head + 1] * state + dot_f32((k_t * weight[head:head + 1]).astype(jnp.bfloat16), v_pair))
        sout_ref[pair] = jnp.where(low, parts[0], parts[1])


def finish_kernel(h_ref, norm_ref, hn_ref, wo_ref, w1_ref, w2_ref, out_ref, acc_scr, in_scr):
    step = pl.program_id(0)
    rows = h_ref.shape[0]

    @pl.when(step == 0)
    def _():
        for start in range(0, h_ref.shape[1], COLS):
            cols = slice(start, start + COLS)
            acc_scr[:, cols] = h_ref[:, cols].astype(jnp.float32) + dot_f32(hn_ref[...], wo_ref[:, cols])
        in_scr[...] = rms_norm(acc_scr[...], norm_ref[...]).astype(jnp.bfloat16)

    for start in range(0, rows, ROWS):
        part = slice(start, start + ROWS)
        hidden = jax.nn.gelu(dot_f32(in_scr[part, :], w1_ref[...]), approximate=True).astype(jnp.bfloat16)
        acc_scr[part, :] += dot_f32(hidden, w2_ref[...])

    @pl.when(step == pl.num_programs(0) - 1)
    def _():
        out_ref[...] = acc_scr[...].astype(jnp.bfloat16)


def attn_kernel(key_dim, q_ref, kt_ref, v_ref, cum_ref, gain_ref, sin_ref, out_ref, sout_ref):
    @pl.when(pl.program_id(1) == 0)
    def _():
        sout_ref[...] = sin_ref[...]

    cum = cum_ref[...]
    chunk = cum.shape[1]
    cum_col = cum.T
    total = cum[:, chunk - 1:]
    wide = sout_ref.shape[2]
    val_dim = wide // 2
    causal = lax.broadcasted_iota(jnp.int32, (chunk, chunk), 0) >= lax.broadcasted_iota(jnp.int32, (chunk, chunk), 1)
    low = lax.broadcasted_iota(jnp.int32, (chunk, wide), 1) < val_dim
    low_s = lax.broadcasted_iota(jnp.int32, (key_dim, wide), 1) < val_dim
    for pair in range(sout_ref.shape[0]):
        v_pair = v_ref[:, pair * wide:(pair + 1) * wide]
        state = sout_ref[pair]
        state_b = state.astype(jnp.bfloat16)
        outs, states = [], []
        for head in (2 * pair, 2 * pair + 1):
            q_head = q_ref[:, head * key_dim:(head + 1) * key_dim]
            k_t = kt_ref[head * key_dim:(head + 1) * key_dim, :]
            row, col = cum_col[:, head:head + 1], cum[head:head + 1]
            decay = jnp.exp(jnp.where(causal, row - col, -jnp.inf))
            weights = (dot_f32(q_head, k_t) * decay).astype(jnp.bfloat16)
            outs.append(dot_f32(weights, v_pair) + dot_f32(q_head, state_b) * jnp.exp(row))
            k_dec = (k_t.astype(jnp.float32) * jnp.exp(total[head:head + 1] - col)).astype(jnp.bfloat16)
            states.append(jnp.exp(total[head:head + 1]) * state + dot_f32(k_dec, v_pair))
        sout_ref[pair] = jnp.where(low_s, states[0], states[1])
        out = jnp.where(low, outs[0], outs[1])
        square = out * out
        low_ms = jnp.sum(jnp.where(low, square, 0.0), axis=1, keepdims=True) * (1.0 / val_dim)
        high_ms = jnp.sum(jnp.where(low, 0.0, square), axis=1, keepdims=True) * (1.0 / val_dim)
        scale = jnp.where(low, lax.rsqrt(low_ms + NORM_EPS), lax.rsqrt(high_ms + NORM_EPS))
        out_ref[:, pair * wide:(pair + 1) * wide] = (out * scale * gain_ref[...]).astype(jnp.bfloat16)


def chain_kernel(n, local_ref, decay_ref, in_ref, out_ref, held, send_sem, recv_sem):
    me = lax.axis_index('seq')
    barrier = pltpu.get_barrier_semaphore()
    groups = send_sem.shape[0]
    size = local_ref.shape[0] // groups

    def copy(group):
        part = pl.ds(group * size, size)
        return pltpu.make_async_remote_copy(
            src_ref=out_ref.at[part], dst_ref=held.at[part],
            send_sem=send_sem.at[group], recv_sem=recv_sem.at[group],
            device_id={'seq': me + 1}, device_id_type=pl.DeviceIdType.MESH)

    @pl.when(me > 0)
    def _():
        pl.semaphore_signal(barrier, inc=1, device_id={'seq': me - 1}, device_id_type=pl.DeviceIdType.MESH)

    @pl.when(me < n - 1)
    def _():
        pl.semaphore_wait(barrier, 1)

    @pl.when(me == 0)
    def _():
        held[...] = jnp.zeros_like(held)

    for group in range(groups):
        part = pl.ds(group * size, size)

        @pl.when(me > 0)
        def _():
            copy(group).wait_recv()

        out_ref[part] = decay_ref[part] * held[part] + local_ref[part]
        in_ref[part] = held[part]

        @pl.when(me < n - 1)
        def _():
            copy(group).start()

    @pl.when(me < n - 1)
    def _():
        for group in range(groups):
            copy(group).wait_send()


def solution(mesh):
    num_stages = mesh.shape['stage']
    num_shards = mesh.shape['seq']
    stage_pairs = [(src, src + 1) for src in range(num_stages - 1)]
    mat_spec = P('stage', None, None)
    vec_spec = P('stage', None)
    weight_specs = (vec_spec, mat_spec, mat_spec, mat_spec, mat_spec, vec_spec, vec_spec, mat_spec, vec_spec, mat_spec, mat_spec)

    def device_program(x_tokens, norm_attn, w_query, w_key, w_value, w_gate, gate_bias, norm_out, w_out, norm_mlp, w_up, w_down):
        stage_idx = lax.axis_index('stage')
        seq_idx = lax.axis_index('seq')
        stacked = (norm_attn, w_query, w_key, w_value, w_gate, gate_bias, norm_out, w_out, norm_mlp, w_up, w_down)
        norm_attn, w_query, w_key, w_value, w_gate, gate_bias, norm_out, w_out, norm_mlp, w_up, w_down = (w[0] for w in stacked)
        num_seqs, tok_len, width = x_tokens.shape
        num_heads = gate_bias.shape[0]
        key_dim = w_query.shape[1] // num_heads
        val_dim = norm_out.shape[0]
        wide = 2 * val_dim
        num_pairs = num_heads // 2
        groups = num_pairs // PAIRS
        rows = tok_len // PIECES
        chunks = rows // CHUNK
        state_shape = (num_pairs, key_dim, wide)
        gain_wide = jnp.tile(norm_out.astype(jnp.float32), 2)[None]
        tri = (jnp.arange(CHUNK)[:, None] <= jnp.arange(CHUNK)[None, :]).astype(jnp.float32)

        kt_block = pl.BlockSpec((2 * PAIRS * key_dim, CHUNK), lambda g, c: (g, c))
        q_block = pl.BlockSpec((CHUNK, 2 * PAIRS * key_dim), lambda g, c: (c, g))
        v_block = pl.BlockSpec((CHUNK, PAIRS * wide), lambda g, c: (c, g))
        cum_block = pl.BlockSpec((2 * PAIRS, CHUNK), lambda g, c: (g, c))
        state_block = pl.BlockSpec((PAIRS, key_dim, wide), lambda g, c: (g, 0, 0))
        state_out = jax.ShapeDtypeStruct(state_shape, jnp.float32)
        params = pltpu.CompilerParams(dimension_semantics=('arbitrary', 'arbitrary'))
        head_rows = num_heads * rows
        key_width, val_width = num_heads * key_dim, num_heads * val_dim
        ffn_dim = w_up.shape[1]
        bf16_out = lambda *shape: jax.ShapeDtypeStruct(shape, jnp.bfloat16)
        whole = lambda *shape: pl.BlockSpec(shape, lambda g: (0,) * len(shape))

        run_project = pl.pallas_call(
            functools.partial(project_kernel, key_dim, CHUNK), grid=(groups,),
            in_specs=[whole(rows, width), whole(1, width), whole(num_heads, width), whole(num_heads, 1), whole(CHUNK, CHUNK),
                      pl.BlockSpec((width, 2 * PAIRS * key_dim), lambda g: (0, g)),
                      pl.BlockSpec((width, 2 * PAIRS * key_dim), lambda g: (0, g)),
                      pl.BlockSpec((width, PAIRS * wide), lambda g: (0, g)),
                      pl.BlockSpec((PAIRS, key_dim, wide), lambda g: (g, 0, 0))],
            out_specs=(pl.BlockSpec((rows, 2 * PAIRS * key_dim), lambda g: (0, g)),
                       pl.BlockSpec((2 * PAIRS * key_dim, rows), lambda g: (g, 0)),
                       pl.BlockSpec((rows, PAIRS * wide), lambda g: (0, g)),
                       pl.BlockSpec((2 * PAIRS, rows), lambda g: (g, 0)),
                       pl.BlockSpec((PAIRS, key_dim, wide), lambda g: (g, 0, 0))),
            out_shape=(bf16_out(rows, key_width), bf16_out(key_width, rows), bf16_out(rows, val_width),
                       jax.ShapeDtypeStruct((num_heads, rows), jnp.float32), state_out),
            scratch_shapes=[pltpu.VMEM((rows, width), jnp.bfloat16), pltpu.VMEM((num_heads, rows), jnp.float32)],
            compiler_params=pltpu.CompilerParams(dimension_semantics=('arbitrary',)), name='project',
            cost_estimate=pl.CostEstimate(flops=2 * rows * width * (2 * key_width + val_width),
                                          bytes_accessed=2 * width * (2 * key_width + val_width), transcendentals=0))
        run_finish = pl.pallas_call(
            finish_kernel, grid=(ffn_dim // HIDDEN,),
            in_specs=[whole(rows, width), whole(1, width), whole(rows, val_width), whole(val_width, width),
                      pl.BlockSpec((width, HIDDEN), lambda g: (0, g)), pl.BlockSpec((HIDDEN, width), lambda g: (g, 0))],
            out_specs=whole(rows, width), out_shape=bf16_out(rows, width),
            scratch_shapes=[pltpu.VMEM((rows, width), jnp.float32), pltpu.VMEM((rows, width), jnp.bfloat16)],
            compiler_params=pltpu.CompilerParams(dimension_semantics=('arbitrary',)), name='finish',
            cost_estimate=pl.CostEstimate(flops=2 * rows * width * (val_width + 2 * ffn_dim),
                                          bytes_accessed=2 * width * (val_width + 2 * ffn_dim), transcendentals=rows * ffn_dim))
        run_attn = pl.pallas_call(
            functools.partial(attn_kernel, key_dim), grid=(groups, chunks),
            in_specs=[q_block, kt_block, v_block, cum_block, pl.BlockSpec((1, wide), lambda g, c: (0, 0)), state_block],
            out_specs=(v_block, state_block),
            out_shape=(jax.ShapeDtypeStruct((rows, num_heads * val_dim), jnp.bfloat16), state_out),
            compiler_params=params, name='chunk_attention',
            cost_estimate=pl.CostEstimate(flops=2 * head_rows * (CHUNK * (key_dim + wide) + 2 * key_dim * wide),
                                          bytes_accessed=12 * rows * num_heads * val_dim, transcendentals=head_rows * CHUNK))
        run_chain = pl.pallas_call(
            functools.partial(chain_kernel, num_shards),
            in_specs=[pl.BlockSpec(memory_space=pltpu.VMEM)] * 2,
            out_specs=(pl.BlockSpec(memory_space=pltpu.VMEM),) * 2,
            out_shape=(state_out, state_out),
            scratch_shapes=[pltpu.VMEM(state_shape, jnp.float32), pltpu.SemaphoreType.DMA((LINKS,)), pltpu.SemaphoreType.DMA((LINKS,))],
            compiler_params=pltpu.CompilerParams(collective_id=0, has_side_effects=True), name='state_chain')

        norm_attn, norm_mlp = norm_attn[None], norm_mlp[None]
        w_gate, gate_bias = w_gate.T, gate_bias[:, None]

        def run_layer(h_pieces, first):
            state = jnp.zeros(state_shape, jnp.float32)
            proj, totals = [], []
            for piece, h_in in enumerate(h_pieces):
                if first is not None:
                    h_in, state = lax.optimization_barrier((h_in, state))
                    h_in = h_pieces[piece] = jnp.where(stage_idx == 0, first[piece], h_in)
                *parts, state = run_project(h_in, norm_attn, w_gate, gate_bias, tri, w_query, w_key, w_value, state)
                proj.append(parts)
                totals.append(jnp.sum(parts[3][:, CHUNK - 1::CHUNK], axis=1))
            decay = jnp.repeat(jnp.exp(sum(totals)).reshape(num_pairs, 1, 2), val_dim, axis=2)
            state, state_last = run_chain(state, decay)
            h_out = []
            for h_in, (q_all, k_t, v_all, cum) in zip(h_pieces, proj):
                head_norm, state = run_attn(q_all, k_t, v_all, cum, gain_wide, state)
                h_out.append(run_finish(h_in, norm_mlp, head_norm, w_out, w_up, w_down))
            return h_out, state_last

        h_ticks, s_ticks = [], []
        h_recv = None
        for tick in range(num_stages + num_seqs - 1):
            first = None
            if tick < num_seqs:
                first = [x_tokens[tick, piece * rows:(piece + 1) * rows] for piece in range(PIECES)]
            if h_recv is None:
                h_recv, first = first, None
            h_out, state_last = run_layer(h_recv, first)
            h_ticks.append(h_out)
            s_ticks.append(state_last)
            if tick < num_stages + num_seqs - 2:
                h_recv = [lax.ppermute(a, 'stage', stage_pairs) for a in h_out]
        s_out = jnp.stack([lax.select_n(stage_idx, *s_ticks[seq:seq + num_stages]) for seq in range(num_seqs)])
        s_out = lax.psum(jnp.where(seq_idx == num_shards - 1, s_out, 0.0), 'seq')
        y_out = jnp.stack([
            jnp.concatenate([lax.select_n(stage_idx, *[h_ticks[seq + stage][piece] for stage in range(num_stages)])
                             for piece in range(PIECES)], axis=0) for seq in range(num_seqs)])
        s_out = s_out.reshape(num_seqs, num_pairs, key_dim, 2, val_dim)
        s_out = jnp.swapaxes(s_out, 2, 3).reshape(num_seqs, num_heads, key_dim, val_dim)
        return y_out[None], s_out[None]

    return jax.shard_map(
        device_program,
        mesh=mesh,
        in_specs=(P('batch', 'seq', None),) + weight_specs,
        out_specs=(P('stage', 'batch', 'seq', None), P('stage', 'batch', None, None, None)),
        check_vma=False,
    )
```

```python
import functools

import jax
import jax.numpy as jnp
from jax import lax
from jax.experimental import pallas as pl
from jax.experimental.pallas import tpu as pltpu
from jax.sharding import PartitionSpec as P

NORM_EPS = 1e-6
CHUNK = 256
PAIRS = 4
ATTN_PAIRS = 8
PIECES = 2
COLS = 256
ROWS = 256
HIDDEN = 1024
LINKS = 8


def rms_norm(values, gain_vec):
    mean_sq = jnp.mean(values * values, axis=-1, keepdims=True)
    return values * lax.rsqrt(mean_sq + NORM_EPS) * gain_vec.astype(jnp.float32)


def dot_f32(lhs, rhs):
    return jnp.dot(lhs, rhs, preferred_element_type=jnp.float32)


def project_kernel(key_dim, chunk, h_ref, norm_ref, wg_ref, bias_ref, tri_ref, wk_ref, wv_ref, sin_ref,
                   u_ref, kt_ref, v_ref, cum_ref, sout_ref, total_ref, cum_scr):
    rows = h_ref.shape[0]
    heads = cum_ref.shape[0]
    group = pl.program_id(0)

    @pl.when(group == 0)
    def _():
        u_ref[...] = rms_norm(h_ref[...].astype(jnp.float32), norm_ref[...]).astype(jnp.bfloat16)
        gate = lax.dot_general(wg_ref[...], u_ref[...], (((1,), (1,)), ((), ())), preferred_element_type=jnp.float32)
        log_decay = jax.nn.log_sigmoid(gate + bias_ref[...])
        for start in range(0, rows, chunk):
            cum_scr[:, start:start + chunk] = jnp.dot(
                log_decay[:, start:start + chunk], tri_ref[...], precision=lax.Precision.HIGHEST,
                preferred_element_type=jnp.float32)

    u_norm = u_ref[...]
    for start in range(0, wv_ref.shape[1], COLS):
        v_ref[:, start:start + COLS] = dot_f32(u_norm, wv_ref[:, start:start + COLS]).astype(jnp.bfloat16)
    for start in range(0, wk_ref.shape[1], COLS):
        k_part = dot_f32(u_norm, wk_ref[:, start:start + COLS]) * key_dim ** -0.5
        kt_ref[start:start + COLS, :] = k_part.T.astype(jnp.bfloat16)
    cum = cum_scr[pl.ds(pl.multiple_of(group * heads, heads), heads), :]
    cum_ref[...] = cum
    total = jnp.zeros((heads, 1), jnp.float32)
    rest = []
    for start in range(rows - chunk, -1, -chunk):
        last = cum[:, start + chunk - 1:start + chunk]
        rest.insert(0, total + (last - cum[:, start:start + chunk]))
        total = total + last
    weight = jnp.exp(jnp.concatenate(rest, axis=1))
    wide = sout_ref.shape[2]
    low = lax.broadcasted_iota(jnp.int32, (key_dim, wide), 1) < wide // 2
    for pair in range(sout_ref.shape[0]):
        total_ref[pair] = jnp.where(low[:1], total[2 * pair:2 * pair + 1], total[2 * pair + 1:2 * pair + 2])
    total = jnp.exp(total)
    for pair in range(sout_ref.shape[0]):
        v_pair = v_ref[:, pair * wide:(pair + 1) * wide]
        state = sin_ref[pair]
        parts = []
        for head in (2 * pair, 2 * pair + 1):
            k_t = kt_ref[head * key_dim:(head + 1) * key_dim, :].astype(jnp.float32)
            parts.append(total[head:head + 1] * state + dot_f32((k_t * weight[head:head + 1]).astype(jnp.bfloat16), v_pair))
        sout_ref[pair] = jnp.where(low, parts[0], parts[1])


def finish_kernel(h_ref, norm_ref, hn_ref, wo_ref, w1_ref, w2_ref, out_ref, acc_scr, in_scr):
    step = pl.program_id(0)
    rows = h_ref.shape[0]

    @pl.when(step == 0)
    def _():
        for start in range(0, h_ref.shape[1], COLS):
            cols = slice(start, start + COLS)
            acc_scr[:, cols] = h_ref[:, cols].astype(jnp.float32) + dot_f32(hn_ref[...], wo_ref[:, cols])
        in_scr[...] = rms_norm(acc_scr[...], norm_ref[...]).astype(jnp.bfloat16)

    for start in range(0, rows, ROWS):
        part = slice(start, start + ROWS)
        hidden = jax.nn.gelu(dot_f32(in_scr[part, :], w1_ref[...]), approximate=True).astype(jnp.bfloat16)
        acc_scr[part, :] += dot_f32(hidden, w2_ref[...])

    @pl.when(step == pl.num_programs(0) - 1)
    def _():
        out_ref[...] = acc_scr[...].astype(jnp.bfloat16)


def attn_kernel(key_dim, q_ref, kt_ref, v_ref, cum_ref, gain_ref, sin_ref, out_ref, sout_ref):
    @pl.when(pl.program_id(1) == 0)
    def _():
        sout_ref[...] = sin_ref[...]

    cum = cum_ref[...]
    chunk = cum.shape[1]
    cum_col = cum.T
    total = cum[:, chunk - 1:]
    wide = sout_ref.shape[2]
    val_dim = wide // 2
    half = chunk // 2
    causal = lax.broadcasted_iota(jnp.int32, (half, half), 0) >= lax.broadcasted_iota(jnp.int32, (half, half), 1)
    low = lax.broadcasted_iota(jnp.int32, (chunk, wide), 1) < val_dim
    low_s = lax.broadcasted_iota(jnp.int32, (key_dim, wide), 1) < val_dim
    low_q = low_s[:1]
    for pair in range(sout_ref.shape[0]):
        v_pair = v_ref[:, pair * wide:(pair + 1) * wide]
        state = sout_ref[pair]
        state_b = jnp.concatenate([jnp.where(low_s, state, 0.0), jnp.where(low_s, 0.0, state)], axis=0).astype(jnp.bfloat16)
        from_state = dot_f32(q_ref[:, 2 * pair * key_dim:2 * (pair + 1) * key_dim], state_b)
        outs, states, rows = [], [], []
        for head in (2 * pair, 2 * pair + 1):
            q_head = q_ref[:, head * key_dim:(head + 1) * key_dim]
            k_t = kt_ref[head * key_dim:(head + 1) * key_dim, :]
            row, col = cum_col[:, head:head + 1], cum[head:head + 1]
            top, bottom, left, right = row[:half], row[half:], col[:, :half], col[:, half:]
            upper = dot_f32(q_head[:half], k_t[:, :half]) * jnp.exp(jnp.where(causal, top - left, -jnp.inf))
            lower = dot_f32(q_head[half:], k_t)
            lower = jnp.concatenate([lower[:, :half] * jnp.exp(bottom - left),
                                     lower[:, half:] * jnp.exp(jnp.where(causal, bottom - right, -jnp.inf))], axis=1)
            outs.append(jnp.concatenate([dot_f32(upper.astype(jnp.bfloat16), v_pair[:half]),
                                         dot_f32(lower.astype(jnp.bfloat16), v_pair)], axis=0))
            k_dec = (k_t.astype(jnp.float32) * jnp.exp(total[head:head + 1] - col)).astype(jnp.bfloat16)
            states.append(dot_f32(k_dec, v_pair))
            rows.append(row)
        keep = jnp.where(low_q, total[2 * pair:2 * pair + 1], total[2 * pair + 1:2 * pair + 2])
        sout_ref[pair] = jnp.exp(keep) * state + jnp.where(low_s, states[0], states[1])
        out = jnp.where(low, outs[0], outs[1]) + from_state * jnp.exp(jnp.where(low, rows[0], rows[1]))
        square = out * out
        low_ms = jnp.sum(jnp.where(low, square, 0.0), axis=1, keepdims=True) * (1.0 / val_dim)
        high_ms = jnp.sum(jnp.where(low, 0.0, square), axis=1, keepdims=True) * (1.0 / val_dim)
        scale = jnp.where(low, lax.rsqrt(low_ms + NORM_EPS), lax.rsqrt(high_ms + NORM_EPS))
        out_ref[:, pair * wide:(pair + 1) * wide] = (out * scale * gain_ref[...]).astype(jnp.bfloat16)


def chain_kernel(n, pieces, *refs):
    u_refs, (wq_ref, local_ref, decay_ref), refs = refs[:pieces], refs[pieces:pieces + 3], refs[pieces + 3:]
    q_refs, (in_ref, out_ref, held, sent, send_sem, recv_sem) = refs[:pieces], refs[pieces:]
    me = lax.axis_index('seq')
    step = pl.program_id(0)
    groups = send_sem.shape[0]
    size = local_ref.shape[0] // groups

    def copy(group):
        part = pl.ds(group * size, size)
        return pltpu.make_async_remote_copy(
            src_ref=sent.at[part], dst_ref=held.at[part],
            send_sem=send_sem.at[group], recv_sem=recv_sem.at[group],
            device_id={'seq': me + 1}, device_id_type=pl.DeviceIdType.MESH)

    @pl.when(step == 0)
    def _():
        barrier = pltpu.get_barrier_semaphore()

        @pl.when(me > 0)
        def _():
            pl.semaphore_signal(barrier, inc=1, device_id={'seq': me - 1}, device_id_type=pl.DeviceIdType.MESH)

        @pl.when(me < n - 1)
        def _():
            pl.semaphore_wait(barrier, 1)

        @pl.when(me == 0)
        def _():
            held[...] = jnp.zeros_like(held)

    for u_ref, q_ref in zip(u_refs, q_refs):
        q_ref[...] = dot_f32(u_ref[...], wq_ref[...]).astype(jnp.bfloat16)

    group = step - me

    @pl.when((group >= 0) & (group < groups))
    def _():
        part = pl.ds(group * size, size)

        @pl.when(me > 0)
        def _():
            copy(group).wait_recv()

        sent[part] = decay_ref[part] * held[part] + local_ref[part]

        @pl.when(me < n - 1)
        def _():
            copy(group).start()

    @pl.when(step == pl.num_programs(0) - 1)
    def _():
        in_ref[...] = held[...]
        out_ref[...] = sent[...]

        @pl.when(me < n - 1)
        def _():
            for group in range(groups):
                copy(group).wait_send()


def solution(mesh):
    num_stages = mesh.shape['stage']
    num_shards = mesh.shape['seq']
    stage_pairs = [(src, src + 1) for src in range(num_stages - 1)]
    mat_spec = P('stage', None, None)
    vec_spec = P('stage', None)
    weight_specs = (vec_spec, mat_spec, mat_spec, mat_spec, mat_spec, vec_spec, vec_spec, mat_spec, vec_spec, mat_spec, mat_spec)

    def device_program(x_tokens, norm_attn, w_query, w_key, w_value, w_gate, gate_bias, norm_out, w_out, norm_mlp, w_up, w_down):
        stage_idx = lax.axis_index('stage')
        seq_idx = lax.axis_index('seq')
        stacked = (norm_attn, w_query, w_key, w_value, w_gate, gate_bias, norm_out, w_out, norm_mlp, w_up, w_down)
        norm_attn, w_query, w_key, w_value, w_gate, gate_bias, norm_out, w_out, norm_mlp, w_up, w_down = (w[0] for w in stacked)
        num_seqs, tok_len, width = x_tokens.shape
        num_heads = gate_bias.shape[0]
        key_dim = w_query.shape[1] // num_heads
        val_dim = norm_out.shape[0]
        wide = 2 * val_dim
        num_pairs = num_heads // 2
        groups = num_pairs // PAIRS
        rows = tok_len // PIECES
        chunks = rows // CHUNK
        state_shape = (num_pairs, key_dim, wide)
        gain_wide = jnp.tile(norm_out.astype(jnp.float32), 2)[None]
        tri = (jnp.arange(CHUNK)[:, None] <= jnp.arange(CHUNK)[None, :]).astype(jnp.float32)

        kt_block = pl.BlockSpec((2 * ATTN_PAIRS * key_dim, CHUNK), lambda g, c: (g, c))
        q_block = pl.BlockSpec((CHUNK, 2 * ATTN_PAIRS * key_dim), lambda g, c: (c, g))
        v_block = pl.BlockSpec((CHUNK, ATTN_PAIRS * wide), lambda g, c: (c, g))
        cum_block = pl.BlockSpec((2 * ATTN_PAIRS, CHUNK), lambda g, c: (g, c))
        state_block = pl.BlockSpec((ATTN_PAIRS, key_dim, wide), lambda g, c: (g, 0, 0))
        state_out = jax.ShapeDtypeStruct(state_shape, jnp.float32)
        params = pltpu.CompilerParams(dimension_semantics=('arbitrary', 'arbitrary'))
        head_rows = num_heads * rows
        key_width, val_width = num_heads * key_dim, num_heads * val_dim
        ffn_dim = w_up.shape[1]
        bf16_out = lambda *shape: jax.ShapeDtypeStruct(shape, jnp.bfloat16)
        whole = lambda *shape: pl.BlockSpec(shape, lambda g: (0,) * len(shape))

        run_project = pl.pallas_call(
            functools.partial(project_kernel, key_dim, CHUNK), grid=(groups,),
            in_specs=[whole(rows, width), whole(1, width), whole(num_heads, width), whole(num_heads, 1), whole(CHUNK, CHUNK),
                      pl.BlockSpec((width, 2 * PAIRS * key_dim), lambda g: (0, g)),
                      pl.BlockSpec((width, PAIRS * wide), lambda g: (0, g)),
                      pl.BlockSpec((PAIRS, key_dim, wide), lambda g: (g, 0, 0))],
            out_specs=(whole(rows, width),
                       pl.BlockSpec((2 * PAIRS * key_dim, rows), lambda g: (g, 0)),
                       pl.BlockSpec((rows, PAIRS * wide), lambda g: (0, g)),
                       pl.BlockSpec((2 * PAIRS, rows), lambda g: (g, 0)),
                       pl.BlockSpec((PAIRS, key_dim, wide), lambda g: (g, 0, 0)),
                       pl.BlockSpec((PAIRS, 1, wide), lambda g: (g, 0, 0))),
            out_shape=(bf16_out(rows, width), bf16_out(key_width, rows), bf16_out(rows, val_width),
                       jax.ShapeDtypeStruct((num_heads, rows), jnp.float32), state_out,
                       jax.ShapeDtypeStruct((num_pairs, 1, wide), jnp.float32)),
            scratch_shapes=[pltpu.VMEM((num_heads, rows), jnp.float32)],
            compiler_params=pltpu.CompilerParams(dimension_semantics=('arbitrary',)), name='project',
            cost_estimate=pl.CostEstimate(flops=2 * rows * width * (key_width + val_width),
                                          bytes_accessed=2 * width * (key_width + val_width), transcendentals=0))
        run_finish = pl.pallas_call(
            finish_kernel, grid=(ffn_dim // HIDDEN,),
            in_specs=[whole(rows, width), whole(1, width), whole(rows, val_width), whole(val_width, width),
                      pl.BlockSpec((width, HIDDEN), lambda g: (0, g)), pl.BlockSpec((HIDDEN, width), lambda g: (g, 0))],
            out_specs=whole(rows, width), out_shape=bf16_out(rows, width),
            scratch_shapes=[pltpu.VMEM((rows, width), jnp.float32), pltpu.VMEM((rows, width), jnp.bfloat16)],
            compiler_params=pltpu.CompilerParams(dimension_semantics=('arbitrary',)), name='finish',
            cost_estimate=pl.CostEstimate(flops=2 * rows * width * (val_width + 2 * ffn_dim),
                                          bytes_accessed=2 * width * (val_width + 2 * ffn_dim), transcendentals=rows * ffn_dim))
        run_attn = pl.pallas_call(
            functools.partial(attn_kernel, key_dim), grid=(num_pairs // ATTN_PAIRS, chunks),
            in_specs=[q_block, kt_block, v_block, cum_block, pl.BlockSpec((1, wide), lambda g, c: (0, 0)), state_block],
            out_specs=(v_block, state_block),
            out_shape=(jax.ShapeDtypeStruct((rows, num_heads * val_dim), jnp.bfloat16), state_out),
            compiler_params=params, name='chunk_attention',
            cost_estimate=pl.CostEstimate(flops=2 * head_rows * (CHUNK * (key_dim + wide) + 2 * key_dim * wide),
                                          bytes_accessed=12 * rows * num_heads * val_dim, transcendentals=head_rows * CHUNK))
        steps = num_shards + LINKS
        cols = key_width // steps
        run_chain = pl.pallas_call(
            functools.partial(chain_kernel, num_shards, PIECES), grid=(steps,),
            in_specs=[whole(rows, width)] * PIECES + [pl.BlockSpec((width, cols), lambda g: (0, g)), whole(*state_shape),
                                                      whole(num_pairs, 1, wide)],
            out_specs=(pl.BlockSpec((rows, cols), lambda g: (0, g)),) * PIECES + (whole(*state_shape),) * 2,
            out_shape=(bf16_out(rows, key_width),) * PIECES + (state_out, state_out),
            scratch_shapes=[pltpu.VMEM(state_shape, jnp.float32), pltpu.VMEM(state_shape, jnp.float32),
                            pltpu.SemaphoreType.DMA((LINKS,)), pltpu.SemaphoreType.DMA((LINKS,))],
            compiler_params=pltpu.CompilerParams(dimension_semantics=('arbitrary',), collective_id=0, has_side_effects=True),
            name='state_chain',
            cost_estimate=pl.CostEstimate(flops=2 * PIECES * rows * width * key_width, bytes_accessed=2 * width * key_width,
                                          transcendentals=0))

        norm_attn, norm_mlp = norm_attn[None], norm_mlp[None]
        w_gate, gate_bias = w_gate.T, gate_bias[:, None]

        def run_layer(h_pieces, first):
            state = jnp.zeros(state_shape, jnp.float32)
            proj, totals = [], []
            for piece, h_in in enumerate(h_pieces):
                if first is not None:
                    h_in, state = lax.optimization_barrier((h_in, state))
                    h_in = h_pieces[piece] = jnp.where(stage_idx == 0, first[piece], h_in)
                *parts, state, total = run_project(h_in, norm_attn, w_gate, gate_bias, tri, w_key, w_value, state)
                proj.append(parts)
                totals.append(total)
            decay = jnp.exp(sum(totals))
            *queries, state, state_last = run_chain(*[part[0] for part in proj], w_query, state, decay)
            h_out = []
            for h_in, q_all, (_, k_t, v_all, cum) in zip(h_pieces, queries, proj):
                head_norm, state = run_attn(q_all, k_t, v_all, cum, gain_wide, state)
                h_out.append(run_finish(h_in, norm_mlp, head_norm, w_out, w_up, w_down))
            return h_out, state_last

        h_ticks, s_ticks = [], []
        h_recv = None
        for tick in range(num_stages + num_seqs - 1):
            first = None
            if tick < num_seqs:
                first = [x_tokens[tick, piece * rows:(piece + 1) * rows] for piece in range(PIECES)]
            if h_recv is None:
                h_recv, first = first, None
            h_out, state_last = run_layer(h_recv, first)
            h_ticks.append(h_out)
            s_ticks.append(state_last)
            if tick < num_stages + num_seqs - 2:
                h_recv = [lax.ppermute(a, 'stage', stage_pairs) for a in h_out]
        s_out = jnp.stack([lax.select_n(stage_idx, *s_ticks[seq:seq + num_stages]) for seq in range(num_seqs)])
        s_out = lax.psum(jnp.where(seq_idx == num_shards - 1, s_out, 0.0), 'seq')
        y_out = jnp.stack([
            jnp.concatenate([lax.select_n(stage_idx, *[h_ticks[seq + stage][piece] for stage in range(num_stages)])
                             for piece in range(PIECES)], axis=0) for seq in range(num_seqs)])
        s_out = s_out.reshape(num_seqs, num_pairs, key_dim, 2, val_dim)
        s_out = jnp.swapaxes(s_out, 2, 3).reshape(num_seqs, num_heads, key_dim, val_dim)
        return y_out[None], s_out[None]

    return jax.shard_map(
        device_program,
        mesh=mesh,
        in_specs=(P('batch', 'seq', None),) + weight_specs,
        out_specs=(P('stage', 'batch', 'seq', None), P('stage', 'batch', None, None, None)),
        check_vma=False,
    )
```
